32 devices in a mesh: rep: 8 (over y, x, core), tp: 4 (over z).
Axes of the slice: x: 2, y: 2, z: 4, core: 2. Of those that a mesh axis runs over, the one named last changes fastest.
Arguments:
- tokens: bfloat16 [4096, 8192], P('rep'), may hold values from -6 to 6
- query_weight: float32 [8192, 8192], P(('rep', 'tp')), may hold values from -0.0625 to 0.0625
- key_weight: float32 [8192, 1024], P(('rep', 'tp')), may hold values from -0.0625 to 0.0625
- value_weight: float32 [8192, 1024], P(('rep', 'tp')), may hold values from -0.0625 to 0.0625
- cache_keys: bfloat16 [256, 128, 1024], P('rep', None, 'tp'), may hold values from -240 to 240
- cache_values: bfloat16 [256, 128, 1024], P('rep', None, 'tp'), may hold values from -6 to 6
- lengths: int32 [8, 2], P('rep'), may hold values from 1 to 2048
- page_table: int32 [8, 2, 16], P('rep'), may hold values from 0 to 31, as said below
Outputs:
- attended: bfloat16 [4096, 8192], P('rep', 'tp')
- new_cache: bfloat16 [2, 4096, 1024], P(None, 'rep', 'tp')
The draws below stay inside these ranges and needn't reach their ends.
Inputs may be any that keep to these rules, and one draw needn't show every extreme that they name: For each group g, the 2 x 16 entries of page_table[g] name each of the group's local pool pages 0 to 31 exactly once.
All inputs are finite; a program needn't handle non-finite values.
Results may differ from the reference program's by a relative error of at most 0.008.
The reference program's roundings to bfloat16 on the way (of `probs`) count: a program that leaves them out, or rounds other values in their place, can miss the bound.
Values may be sent and summed in bfloat16 or wider, within the bound.
No kernel may reach another device: no remote copies, remote signals or barrier semaphores. Data moves between devices by JAX's collectives and lax.ppermute only.
A program may use at most 192 MiB of HBM per device.

```python
import jax
import jax.numpy as jnp
from jax import lax

D = 8192
HEADS = 64
KV_HEADS = 8
HEAD_DIM = 128
SEQS = 2
NEW = 256
PAGE = 128
PAGES_SEQ = 16
REPS = 8
TOK = 512
MAXLEN = 2048
POOL = 32


def draw_cache_keys(key, part):
    shape = (REPS * POOL, PAGE, KV_HEADS * HEAD_DIM)
    base = jnp.clip(jax.random.normal(jax.random.fold_in(key, 11), shape, jnp.float32), -4.0, 4.0)
    return base.astype(jnp.bfloat16)


def draw_page_table(key, part):
    keys = jax.random.split(jax.random.fold_in(key, 21), REPS)
    orders = jax.vmap(lambda single: jax.random.permutation(single, POOL))(keys)
    return orders.astype(jnp.int32).reshape(REPS, SEQS, PAGES_SEQ)


def touch_ends(entries, rng, low, largest):
    spot = [jax.random.randint(jax.random.fold_in(rng, axis), (), 0, length) for axis, length in enumerate(entries.shape)]
    longest = entries.shape.index(max(entries.shape))
    beside = spot[:longest] + [(spot[longest] + 1) % entries.shape[longest]] + spot[longest + 1:]
    return entries.at[tuple(spot)].set(low).at[tuple(beside)].set(largest)


def block_levels(rng, extent, shards, smallest, top_value):
    factor_of, own = 1.0, jax.random.fold_in(rng, 6)
    for axis_at, shards_of in shards:
        steps = jnp.exp(jax.random.uniform(jax.random.fold_in(own, axis_at), (shards_of,), jnp.float32, smallest / len(shards), top_value / len(shards)))
        factor_of = factor_of * jnp.repeat(steps, extent[axis_at] // shards_of).reshape([-1 if axis == axis_at else 1 for axis in range(len(extent))])
    return factor_of


def gaussian(stream_key, dims, deviation, reach, shards=(), held_as=jnp.bfloat16):
    level = block_levels(stream_key, dims, shards, -0.22, 0.18) if shards else 1.0
    values = jax.random.normal(stream_key, dims, jnp.float32) * deviation * level
    return jnp.minimum(jnp.maximum(values, -reach), reach).astype(held_as)


def setup_inputs(seed: int = 0) -> dict:
    splits = jax.random.split(jax.random.key(seed), 9)
    tokens = gaussian(splits[0], (REPS * TOK, D), 1.0, 6.0, ((0, 8),))
    query_weight = gaussian(splits[1], (D, HEADS * HEAD_DIM), D ** -0.5, 0.0625, ((0, 32),), jnp.float32)
    key_weight = gaussian(splits[2], (D, KV_HEADS * HEAD_DIM), D ** -0.5, 0.0625, ((0, 32),), jnp.float32)
    value_weight = gaussian(splits[3], (D, KV_HEADS * HEAD_DIM), D ** -0.5, 0.0625, ((0, 32),), jnp.float32)
    cache_keys = draw_cache_keys(jax.random.fold_in(splits[8], 71), 0)
    cache_values = gaussian(splits[5], (REPS * POOL, PAGE, KV_HEADS * HEAD_DIM), 1.0, 6.0, ((0, 8), (2, 4)))
    lengths = touch_ends(jax.random.randint(splits[6], (REPS, SEQS), 1, MAXLEN + 1), jax.random.fold_in(splits[6], 1), 1, MAXLEN).astype(jnp.int32)
    page_table = draw_page_table(jax.random.fold_in(splits[8], 71), 0)
    return dict(tokens=tokens, query_weight=query_weight, key_weight=key_weight, value_weight=value_weight, cache_keys=cache_keys, cache_values=cache_values, lengths=lengths, page_table=page_table)


ROPE_THETA = 500000.0


def rotate(vectors, positions):
    half_dim = HEAD_DIM // 2
    frequency = ROPE_THETA ** (-2.0 * jnp.arange(half_dim, dtype=jnp.float32) / HEAD_DIM)
    angles = positions.astype(jnp.float32)[:, None] * frequency[None, :]
    cosine_part = jnp.cos(angles)[:, None, :]
    sine_part = jnp.sin(angles)[:, None, :]
    first_half = vectors[..., :half_dim]
    second_half = vectors[..., half_dim:]
    return jnp.concatenate([first_half * cosine_part - second_half * sine_part, second_half * cosine_part + first_half * sine_part], axis=-1)


def reference(tokens, query_weight, key_weight, value_weight, cache_keys, cache_values, lengths, page_table):
    query_bf = query_weight.astype(jnp.bfloat16)
    key_bf = key_weight.astype(jnp.bfloat16)
    value_bf = value_weight.astype(jnp.bfloat16)
    group_size = HEADS // KV_HEADS
    scale = 1.0 / (HEAD_DIM ** 0.5)
    key_pool = cache_keys.reshape(REPS, POOL, PAGE, KV_HEADS * HEAD_DIM)
    value_pool = cache_values.reshape(REPS, POOL, PAGE, KV_HEADS * HEAD_DIM)

    def one_group(items):
        group_tokens, pool_keys, pool_values, group_lengths, group_pages = items
        raw_query = jnp.dot(group_tokens, query_bf, preferred_element_type=jnp.float32)
        raw_key = jnp.dot(group_tokens, key_bf, preferred_element_type=jnp.float32)
        raw_value = jnp.dot(group_tokens, value_bf, preferred_element_type=jnp.float32)
        positions = (group_lengths[:, None] + jnp.arange(NEW, dtype=jnp.int32)[None, :]).reshape(TOK)
        queries = rotate(raw_query.reshape(TOK, HEADS, HEAD_DIM), positions).astype(jnp.bfloat16)
        new_keys = rotate(raw_key.reshape(TOK, KV_HEADS, HEAD_DIM), positions).astype(jnp.bfloat16)
        new_values = raw_value.astype(jnp.bfloat16).reshape(TOK, KV_HEADS, HEAD_DIM)

        def one_sequence(inner):
            seq_queries, seq_keys, seq_values, page_rows, length = inner
            old_keys = pool_keys[page_rows].reshape(MAXLEN, KV_HEADS, HEAD_DIM)
            old_values = pool_values[page_rows].reshape(MAXLEN, KV_HEADS, HEAD_DIM)
            all_keys = jnp.concatenate([old_keys, seq_keys], axis=0).astype(jnp.float32)
            all_values = jnp.concatenate([old_values, seq_values], axis=0).astype(jnp.float32)
            grouped = seq_queries.reshape(NEW, KV_HEADS, group_size, HEAD_DIM).astype(jnp.float32)
            scores = jnp.einsum("nkgd,mkd->kgnm", grouped, all_keys) * scale
            key_index = jnp.arange(MAXLEN + NEW, dtype=jnp.int32)[None, :]
            query_index = jnp.arange(NEW, dtype=jnp.int32)[:, None]
            visible = jnp.where(key_index < MAXLEN, key_index < length, key_index - MAXLEN <= query_index)
            scores = jnp.where(visible[None, None], scores, -1e30)
            maxima = jnp.max(scores, axis=-1, keepdims=True)
            expons = jnp.exp(scores - maxima)
            probs = (expons / jnp.sum(expons, axis=-1, keepdims=True)).astype(jnp.bfloat16)
            output = jnp.einsum("kgnm,mkd->nkgd", probs.astype(jnp.float32), all_values)
            return output.astype(jnp.bfloat16).reshape(NEW, HEADS * HEAD_DIM)

        attended = lax.map(one_sequence, (queries.reshape(SEQS, NEW, HEADS, HEAD_DIM), new_keys.reshape(SEQS, NEW, KV_HEADS, HEAD_DIM), new_values.reshape(SEQS, NEW, KV_HEADS, HEAD_DIM), group_pages, group_lengths))
        return attended.reshape(TOK, HEADS * HEAD_DIM), new_keys.reshape(TOK, KV_HEADS * HEAD_DIM), new_values.reshape(TOK, KV_HEADS * HEAD_DIM)

    attended, key_rows, value_rows = lax.map(one_group, (tokens.reshape(REPS, TOK, D), key_pool, value_pool, lengths, page_table))
    new_cache = jnp.stack([key_rows.reshape(REPS * TOK, KV_HEADS * HEAD_DIM), value_rows.reshape(REPS * TOK, KV_HEADS * HEAD_DIM)])
    return attended.reshape(REPS * TOK, HEADS * HEAD_DIM), new_cache
```

```python
import functools

import jax
import jax.numpy as jnp
from jax import lax
from jax.experimental import pallas as pl
from jax.experimental.pallas import tpu as pltpu
from jax.sharding import PartitionSpec as P

HEADS = 64
KV_HEADS = 8
HEAD_DIM = 128
SEQS = 2
NEW = 256
TOK = 512
MAXLEN = 2048
ROPE_THETA = 500000.0
KEY_BLOCK = 512
VMEM_LIMIT = 56 * 1024 * 1024
BF = jnp.bfloat16

HEAD_CHUNKS = (1, 3, 3, 1)
OWN_ORDER = (0, 1, 2, 3)


def plain_rotate(vectors, positions):
    half_dim = HEAD_DIM // 2
    frequency = ROPE_THETA ** (-2.0 * jnp.arange(half_dim, dtype=jnp.float32) / HEAD_DIM)
    angles = positions.astype(jnp.float32)[:, None] * frequency[None, :]
    cosine_part = jnp.cos(angles)[:, None, :]
    sine_part = jnp.sin(angles)[:, None, :]
    first_half = vectors[..., :half_dim]
    second_half = vectors[..., half_dim:]
    return jnp.concatenate(
        [
            first_half * cosine_part - second_half * sine_part,
            second_half * cosine_part + first_half * sine_part,
        ],
        axis=-1,
    )


def plain(
    tokens, query_weight, key_weight, value_weight, cache_keys, cache_values, lengths, page_table
):
    weights = (
        query_weight.astype(jnp.bfloat16),
        key_weight.astype(jnp.bfloat16),
        value_weight.astype(jnp.bfloat16),
    )
    slabs = (
        lax.all_to_all(weights[0], "tp", split_axis=1, concat_axis=0, tiled=True),
        lax.all_to_all(weights[1], "tp", split_axis=1, concat_axis=0, tiled=True),
        lax.all_to_all(weights[2], "tp", split_axis=1, concat_axis=0, tiled=True),
    )
    pieces = (
        lax.all_gather(slabs[0], "rep", axis=0, tiled=True),
        lax.all_gather(slabs[1], "rep", axis=0, tiled=True),
        lax.all_gather(slabs[2], "rep", axis=0, tiled=True),
    )
    raw_query, raw_key, raw_value = tuple(
        (jnp.dot(tokens, piece, preferred_element_type=jnp.float32) for piece in pieces)
    )
    kv_local = raw_key.shape[1] // HEAD_DIM
    group_size = HEADS // KV_HEADS
    scale = 1.0 / HEAD_DIM**0.5
    seq_lengths = lengths[0]
    positions = (seq_lengths[:, None] + jnp.arange(NEW, dtype=jnp.int32)[None, :]).reshape(TOK)
    queries = plain_rotate(raw_query.reshape(TOK, kv_local * group_size, HEAD_DIM), positions).astype(
        jnp.bfloat16
    )
    new_keys = plain_rotate(raw_key.reshape(TOK, kv_local, HEAD_DIM), positions).astype(jnp.bfloat16)
    new_values = raw_value.astype(jnp.bfloat16).reshape(TOK, kv_local, HEAD_DIM)

    def one_sequence(inner):
        seq_queries, seq_keys, seq_values, page_rows, length = inner
        old_keys = cache_keys[page_rows].reshape(MAXLEN, kv_local, HEAD_DIM)
        old_values = cache_values[page_rows].reshape(MAXLEN, kv_local, HEAD_DIM)
        all_keys = jnp.concatenate([old_keys, seq_keys], axis=0)
        all_values = jnp.concatenate([old_values, seq_values], axis=0)
        grouped = seq_queries.reshape(NEW, kv_local, group_size, HEAD_DIM)
        scores = (
            jnp.einsum("nkgd,mkd->kgnm", grouped, all_keys, preferred_element_type=jnp.float32)
            * scale
        )
        key_index = jnp.arange(MAXLEN + NEW, dtype=jnp.int32)[None, :]
        query_index = jnp.arange(NEW, dtype=jnp.int32)[:, None]
        visible = jnp.where(
            key_index < MAXLEN, key_index < length, key_index - MAXLEN <= query_index
        )
        scores = jnp.where(visible[None, None], scores, -1e30)
        maxima = jnp.max(scores, axis=-1, keepdims=True)
        expons = jnp.exp(scores - maxima)
        probs = (expons / jnp.sum(expons, axis=-1, keepdims=True)).astype(jnp.bfloat16)
        output = jnp.einsum("kgnm,mkd->nkgd", probs, all_values, preferred_element_type=jnp.float32)
        return output.astype(jnp.bfloat16).reshape(NEW, kv_local * group_size * HEAD_DIM)

    attended = lax.map(
        one_sequence,
        (
            queries.reshape(SEQS, NEW, kv_local * group_size, HEAD_DIM),
            new_keys.reshape(SEQS, NEW, kv_local, HEAD_DIM),
            new_values.reshape(SEQS, NEW, kv_local, HEAD_DIM),
            page_table[0],
            seq_lengths,
        ),
    )
    new_cache = jnp.stack(
        [new_keys.reshape(TOK, kv_local * HEAD_DIM), new_values.reshape(TOK, kv_local * HEAD_DIM)]
    )
    return (attended.reshape(TOK, kv_local * group_size * HEAD_DIM), new_cache)


def rotate(v, cos, sin):
    half = HEAD_DIM // 2
    swapped = jnp.concatenate([v[:, half:], v[:, :half]], axis=1)
    return v * cos + swapped * sin


def pack_kernel(jobs, n_recv, starts_ref, *refs):
    weights, received = refs[:3], refs[3 : 3 + n_recv]
    outs = refs[3 + n_recv : 3 + n_recv + len(jobs)]
    buf, sems = refs[-2:]
    flat, at = [], 0
    for out, pieces in zip(outs, jobs):
        for row, col, width, source, begin in pieces:
            if source >= 3:
                continue
            src = weights[source].at[:, pl.ds(pl.multiple_of(starts_ref[begin], 128), width)]
            copy = pltpu.make_async_copy(src, buf.at[:, pl.ds(at, width)], sems.at[len(flat)])
            copy.start()
            flat.append((copy, out, row, col, width, at))
            at += width
    rows = buf.shape[0]
    for out, pieces in zip(outs, jobs):
        for row, col, width, source, begin in pieces:
            if source >= 3:
                out[row : row + rows, col : col + width] = received[source - 3][:, begin : begin + width]
    for copy, out, row, col, width, at in flat:
        copy.wait()
        out[row : row + rows, col : col + width] = buf[:, at : at + width].astype(BF)


def pack(jobs, shapes, starts, weights, received):
    n = sum(1 for pieces in jobs for piece in pieces if piece[3] < 3)
    total = sum(piece[2] for pieces in jobs for piece in pieces if piece[3] < 3)
    rows = weights[0].shape[0]
    return pl.pallas_call(
        functools.partial(pack_kernel, jobs, len(received)),
        out_shape=[jax.ShapeDtypeStruct(shape, BF) for shape in shapes],
        grid_spec=pltpu.PrefetchScalarGridSpec(
            num_scalar_prefetch=1,
            grid=(1,),
            in_specs=[pl.BlockSpec(memory_space=pl.ANY)] * 3
            + [pl.BlockSpec(a.shape, lambda i, _: (0, 0)) for a in received],
            out_specs=[pl.BlockSpec(shape, lambda i, _: (0, 0)) for shape in shapes],
            scratch_shapes=[pltpu.VMEM((rows, total), jnp.float32), pltpu.SemaphoreType.DMA((n,))],
        ),
        compiler_params=pltpu.CompilerParams(vmem_limit_bytes=VMEM_LIMIT),
        cost_estimate=pl.CostEstimate(flops=1000000, bytes_accessed=rows * total * 6, transcendentals=0),
    )(starts, *weights, *received)


def move_kernel(jobs, *refs):
    n_in = 1 + max(job[0] for job in jobs)
    ins, outs, sems = refs[:n_in], refs[n_in:-1], refs[-1]
    copies = []
    for k, (source, first, rows, target, to) in enumerate(jobs):
        copies.append(
            pltpu.make_async_copy(
                ins[source].at[pl.ds(first, rows)], outs[target].at[pl.ds(to, rows)], sems.at[k]
            )
        )
        copies[-1].start()
    for copy in copies:
        copy.wait()


def move(jobs, arrays, shapes):
    return pl.pallas_call(
        functools.partial(move_kernel, jobs),
        out_shape=[jax.ShapeDtypeStruct(shape, BF) for shape in shapes],
        in_specs=[pl.BlockSpec(memory_space=pl.ANY)] * len(arrays),
        out_specs=[pl.BlockSpec(memory_space=pltpu.VMEM)] * len(shapes),
        scratch_shapes=[pltpu.SemaphoreType.DMA((len(jobs),))],
        compiler_params=pltpu.CompilerParams(vmem_limit_bytes=16 * 1024 * 1024),
        cost_estimate=pl.CostEstimate(
            flops=1000000, bytes_accessed=sum(4 * a * b for a, b in shapes), transcendentals=0
        ),
    )(*arrays)


def lanes(x):
    return [x[:, i * 128 : (i + 1) * 128] for i in range(x.shape[1] // 128)]


def spread(column):
    return jnp.broadcast_to(column, (column.shape[0], 128))


def order_kernel(shard, order_ref, theirs_ref, mine_ref, out_ref, sems):
    i = pl.program_id(0)
    rows, depth = out_ref.shape
    half = pl.num_programs(0) // 2

    def copies(ref, first):
        for k in range(depth // shard):
            src = ref.at[pl.ds(first, rows), pl.ds(pl.multiple_of(order_ref[k] * shard, shard), shard)]
            yield pltpu.make_async_copy(src, out_ref.at[:, pl.ds(k * shard, shard)], sems.at[k])

    @pl.when(i < half)
    def _():
        for copy in copies(theirs_ref, i * rows):
            copy.start()

    @pl.when(i >= half)
    def _():
        for copy in copies(mine_ref, (i - half) * rows):
            copy.start()

    for copy in copies(mine_ref, 0):
        copy.wait()


def chunk_kernel(places, heads, with_kv, block, len_ref, tok_ref, cos_ref, sin_ref, ok_ref, ov_ref, *refs):
    if with_kv:
        weights, refs = refs[: len(places)], refs[len(places) :]
        theirs_ref, mine_ref, fresh_ref = refs[:3]
        refs = refs[3:]
    else:
        fresh_ref, weights, refs = refs[0], refs[1 : 1 + len(places)], refs[1 + len(places) :]
        theirs_ref, mine_ref = refs[:2]
        refs = refs[2:]
    q_ref, e_ref, m_ref, l_ref, top_ref, acc_ref = refs
    i = pl.program_id(0)
    new = tok_ref.shape[0]
    length = len_ref[i]
    blocks = (length + block - 1) // block
    factor = (1.0 / HEAD_DIM**0.5) * 1.4426950408889634
    nt = (((1,), (1,)), ((), ()))

    raw = None
    for place, ref in zip(places, weights):
        part = jnp.dot(tok_ref[:, place : place + ref.shape[0]], ref[...], preferred_element_type=jnp.float32)
        raw = part if raw is None else raw + part
    raw = [raw[:, h * HEAD_DIM : (h + 1) * HEAD_DIM] for h in range(raw.shape[1] // HEAD_DIM)]
    if with_kv:
        fresh_ref[0] = rotate(raw[0], cos_ref[...], sin_ref[...]).astype(BF)
        fresh_ref[1] = raw[1].astype(BF)
        raw = raw[2:]
    for h in range(heads):
        q_ref[h * new : (h + 1) * new, :] = rotate(raw[h], cos_ref[...], sin_ref[...]).astype(BF)

    s = lax.dot_general(q_ref[...], fresh_ref[0], nt, preferred_element_type=jnp.float32)
    row = lax.broadcasted_iota(jnp.int32, s.shape, 0) % new
    col = lax.broadcasted_iota(jnp.int32, s.shape, 1)
    parts = lanes(jnp.where(col <= row, s, -1e30))
    m = functools.reduce(jnp.maximum, parts)
    es = [jnp.exp2((c - m) * factor) for c in parts]
    for j, e in enumerate(es):
        e_ref[0, :, j * 128 : (j + 1) * 128] = e
    m_ref[0] = m
    l_ref[...] = sum(es)

    @pl.loop(0, blocks)
    def _(b):
        start = pl.multiple_of(b * block, block)
        s = lax.dot_general(q_ref[...], ok_ref[0, pl.ds(start, block), :], nt, preferred_element_type=jnp.float32)
        at = lax.broadcasted_iota(jnp.int32, s.shape, 1)
        parts = lanes(jnp.where(at < length - start, s, -1e30))
        before = m_ref[b]
        m = functools.reduce(jnp.maximum, parts, before)
        es = [jnp.exp2((c - m) * factor) for c in parts]
        for j, e in enumerate(es):
            e_ref[b + 1, :, j * 128 : (j + 1) * 128] = e
        m_ref[b + 1] = m
        l_ref[...] = l_ref[...] * jnp.exp2((before - m) * factor) + sum(es)

    last = m_ref[blocks]
    top = spread(jnp.max(last, axis=1, keepdims=True))
    total = jnp.sum(l_ref[...] * jnp.exp2((last - top) * factor), axis=1, keepdims=True)
    top_ref[...] = top
    inverse = spread(1.0 / total)
    l_ref[...] = inverse

    def probs(slot, n):
        scale = jnp.exp2((m_ref[slot] - top_ref[...]) * factor) * l_ref[...]
        return jnp.concatenate(
            [(e_ref[slot, :, j * 128 : (j + 1) * 128] * scale).astype(BF) for j in range(n)], axis=1
        )

    acc_ref[...] = jnp.dot(probs(0, new // 128), fresh_ref[1], preferred_element_type=jnp.float32)

    @pl.loop(0, blocks)
    def _(b):
        start = pl.multiple_of(b * block, block)
        acc_ref[...] += jnp.dot(
            probs(b + 1, block // 128), ov_ref[0, pl.ds(start, block), :], preferred_element_type=jnp.float32
        )

    def write(out_ref):
        for h in range(heads):
            out_ref[:, h * HEAD_DIM : (h + 1) * HEAD_DIM] = acc_ref[h * new : (h + 1) * new, :].astype(BF)

    half = pl.num_programs(0) // 2
    pl.when(i < half)(lambda: write(theirs_ref))
    pl.when(i >= half)(lambda: write(mine_ref))


def by_core(R, T, tokens, query_weight, key_weight, value_weight, cache_keys, cache_values, lengths, page_table):
    tok_rows, depth = tokens.shape
    shard = query_weight.shape[0]
    seqs = lengths.shape[1]
    new = tok_rows // seqs
    q_local = query_weight.shape[1] // T
    q_core = q_local // 2
    kv_width = key_weight.shape[1] // T
    r, z = lax.axis_index("rep"), lax.axis_index("tp")
    core = r % 2
    max_len = cache_keys.shape[1] * page_table.shape[2]

    def xor(a, bit):
        return lax.ppermute(a, "rep", [(i, i ^ bit) for i in range(R)])

    head_chunks = HEAD_CHUNKS
    widths = [(n + 2 * (c == 0)) * HEAD_DIM for c, n in enumerate(head_chunks)]
    firsts = [sum(widths[:c]) for c in range(len(widths))]
    own_firsts, col = {}, 0
    for c in OWN_ORDER:
        own_firsts[c] = col
        col += widths[c]
    whole = sum(widths)
    n_chunks = len(widths)

    starts = []
    for s in range(T):
        target = (z + s) % T
        for h in (core, 1 - core):
            starts += [target * q_local + h * q_core, target * kv_width + h * HEAD_DIM, target * kv_width + h * HEAD_DIM]
    for s in range(T):
        target = (z + s) % T
        for h in (core, 1 - core):
            base = target * q_local + h * q_core
            starts += [base + firsts[c] - 2 * HEAD_DIM if c else base for c in range(n_chunks)]
    starts = jnp.stack(starts).astype(jnp.int32)
    weights = (query_weight, key_weight, value_weight)

    def pieces(s, other, c, row, col):
        base, q_base = 3 * (2 * s + other), 6 * T + n_chunks * (2 * s + other)
        if c:
            return [(row, col, widths[c], 0, q_base + c)]
        return [
            (row, col, HEAD_DIM, 1, base + 1),
            (row, col + HEAD_DIM, HEAD_DIM, 2, base + 2),
            (row, col + 2 * HEAD_DIM, widths[0] - 2 * HEAD_DIM, 0, q_base),
        ]

    def all_chunks(s, other, row, col):
        return [p for c in range(n_chunks) for p in pieces(s, other, c, row, col + own_firsts[c])]

    send_a = pack([all_chunks(0, 1, 0, 0)], [(shard, whole)], starts, weights, [])[0]
    got_a = xor(send_a, 1)

    def their_half(chunks):
        job, col, place = [], 0, {}
        for c in chunks:
            for s in range(1, T):
                job += pieces(s, 1, c, 0, col)
                place[s, c] = col
                col += widths[c]
        return pack([job], [(shard, col)], starts, weights, [])[0], place

    def to_send(got, place):
        jobs, shapes = [], []
        for s, c in place:
            jobs.append(pieces(s, 0, c, 0, 0) + [(shard, 0, widths[c], 3, place[s, c])])
            shapes.append((2 * shard, widths[c]))
        return dict(zip(place, pack(jobs, shapes, starts, weights, [got])))

    send_b, place_b = their_half([0])
    got_b = xor(send_b, 1)
    own = pack([all_chunks(0, 0, 0, 0) + [(shard, 0, whole, 3, 0)]], [(2 * shard, whole)], starts, weights, [got_a])[0]
    ready = to_send(got_b, place_b)
    send_c, place_c = their_half(range(1, n_chunks))
    got_c = xor(send_c, 1)
    ready.update(to_send(got_c, place_c))

    def over_tp(c):
        got = []
        for s in range(1, T):
            got.append(lax.ppermute(ready[s, c], "tp", [(t, (t + s) % T) for t in range(T)]))
        rows = got[0].shape[0]
        jobs = [(k, 0, rows, 0, k * rows) for k in range(T - 1)]
        return move(jobs, got, [((T - 1) * rows, widths[c])])[0]

    def gather(piece):
        by_x, by_y = xor(piece, 2), xor(piece, 4)
        n = piece.shape[0] // 2
        jobs = [(0, 0, n, 0, 0), (1, n, n, 1, 0)]
        low, high = move(jobs, [by_y, by_x], [(n, piece.shape[1])] * 2)
        far = [(6, 0, xor(low, 2)), (6, n, xor(high, 4))]
        return [(0, 0, piece), (2, 0, by_x), (4, 0, by_y), *far]

    own_all = gather(own)
    rest_all = [gather(over_tp(c)) for c in range(n_chunks)]

    their_tokens = xor(tokens, 1)
    seq_lengths = jnp.concatenate([xor(lengths, 1)[0], lengths[0]])
    old = jnp.stack(
        [a[page_table[0]].reshape(seqs, max_len, kv_width) for a in (cache_keys, cache_values)]
    )
    mine_old = lax.dynamic_slice_in_dim(old, core * HEAD_DIM, HEAD_DIM, 3)
    their_old = xor(lax.dynamic_slice_in_dim(old, (1 - core) * HEAD_DIM, HEAD_DIM, 3), 1)
    old_keys, old_values = [jnp.concatenate([their_old[k], mine_old[k]], axis=0) for k in range(2)]

    order, place = [], {}
    for shifts in ([0], list(range(1, T))):
        for d in range(0, R, 2):
            place[d, shifts[0]] = len(order) * shard
            order += [(r ^ (d + e)) * T + (z - s) % T for s in shifts for e in range(2)]
    order = jnp.stack(order).astype(jnp.int32)
    rows_all = 2 * tok_rows
    params = pltpu.CompilerParams(vmem_limit_bytes=VMEM_LIMIT)
    call = pl.pallas_call(
        functools.partial(order_kernel, shard),
        out_shape=jax.ShapeDtypeStruct((rows_all, depth), BF),
        grid_spec=pltpu.PrefetchScalarGridSpec(
            num_scalar_prefetch=1,
            grid=(2 * seqs,),
            in_specs=[pl.BlockSpec(memory_space=pl.ANY)] * 2,
            out_specs=pl.BlockSpec((new, depth), lambda i, _: (i, 0)),
            scratch_shapes=[pltpu.SemaphoreType.DMA((depth // shard,))],
        ),
        compiler_params=params,
        cost_estimate=pl.CostEstimate(flops=1000000, bytes_accessed=4 * rows_all * depth, transcendentals=0),
        name="order_tokens",
    )
    tok = call(order, their_tokens, tokens)

    half = HEAD_DIM // 2
    frequency = ROPE_THETA ** (-2.0 * jnp.arange(half, dtype=jnp.float32) / HEAD_DIM)
    positions = (seq_lengths[:, None] + jnp.arange(new, dtype=jnp.int32)[None, :]).reshape(rows_all)
    angles = positions.astype(jnp.float32)[:, None] * frequency[None, :]
    cos, sin = jnp.cos(angles), jnp.sin(angles)
    cos, sin = jnp.concatenate([cos, cos], axis=1), jnp.concatenate([-sin, sin], axis=1)

    def attend(c, fresh):
        n = head_chunks[c]
        width = n * HEAD_DIM
        with_kv = c == 0
        block = KEY_BLOCK if n > 1 else 2 * KEY_BLOCK
        slots = max_len // block + 1
        specs, arrays, places = [], [], []
        for s, first, parts in ((0, own_firsts[c], own_all), (1, 0, rest_all[c])):
            for d, o, a in parts:
                specs.append(
                    pl.BlockSpec((a.shape[0], widths[c]), functools.partial(lambda k, *_: (0, k), first // widths[c]))
                )
                arrays.append(a)
                places.append(place[d, s] + o)
        row = lambda i, *_: (i, 0)
        out_shape = [jax.ShapeDtypeStruct((tok_rows, width), BF)] * 2
        out_specs = [
            pl.BlockSpec((new, width), lambda i, *_: (jnp.minimum(i, seqs - 1), 0)),
            pl.BlockSpec((new, width), lambda i, *_: (jnp.maximum(i - seqs, 0), 0)),
        ]
        fresh_spec = pl.BlockSpec((2, new, HEAD_DIM), lambda i, *_: (0, i, 0))
        if with_kv:
            out_shape.append(jax.ShapeDtypeStruct((2, rows_all, HEAD_DIM), BF))
            out_specs.append(fresh_spec)
        call = pl.pallas_call(
            functools.partial(chunk_kernel, places, n, with_kv, block),
            out_shape=out_shape,
            grid_spec=pltpu.PrefetchScalarGridSpec(
                num_scalar_prefetch=1,
                grid=(2 * seqs,),
                in_specs=[
                    pl.BlockSpec((new, depth), row),
                    pl.BlockSpec((new, HEAD_DIM), row),
                    pl.BlockSpec((new, HEAD_DIM), row),
                    pl.BlockSpec((1, max_len, HEAD_DIM), lambda i, *_: (i, 0, 0)),
                    pl.BlockSpec((1, max_len, HEAD_DIM), lambda i, *_: (i, 0, 0)),
                    *([] if with_kv else [fresh_spec]),
                    *specs,
                ],
                out_specs=out_specs,
                scratch_shapes=[
                    pltpu.VMEM((n * new, HEAD_DIM), BF),
                    pltpu.VMEM((slots, n * new, block), jnp.float32),
                    pltpu.VMEM((slots, n * new, 128), jnp.float32),
                    pltpu.VMEM((n * new, 128), jnp.float32),
                    pltpu.VMEM((n * new, 128), jnp.float32),
                    pltpu.VMEM((n * new, 128), jnp.float32),
                ],
            ),
            compiler_params=params,
            cost_estimate=pl.CostEstimate(
                flops=2 * rows_all * width * (depth + 2 * (max_len + new)),
                bytes_accessed=(rows_all + width) * depth * 2,
                transcendentals=rows_all * n * (max_len + new),
            ),
        )
        extra = () if with_kv else (fresh,)
        return call(seq_lengths, tok, cos, sin, old_keys, old_values, *extra, *arrays)

    out, at, fresh = jnp.zeros((tok_rows, q_local), BF), 0, None
    for c in range(n_chunks):
        theirs, mine, *rest = attend(c, fresh)
        if rest:
            fresh = rest[0]
            back = xor(fresh[:, :tok_rows], 1)
            kept = fresh[:, tok_rows:]
            new_cache = jnp.concatenate(
                [jnp.where(core == 0, kept, back), jnp.where(core == 0, back, kept)], axis=2
            )
        theirs = xor(theirs, 1)
        out = lax.dynamic_update_slice(out, mine, (0, core * q_core + at))
        out = lax.dynamic_update_slice(out, theirs, (0, (1 - core) * q_core + at))
        at += head_chunks[c] * HEAD_DIM
    return out, new_cache


def per_device(R, T, *args):
    _, query_weight, key_weight = args[:3]
    heads = query_weight.shape[1] // T // HEAD_DIM
    kv = key_weight.shape[1] // T // HEAD_DIM
    if R == 8 and kv == 2 and heads == 16:
        return by_core(R, T, *args)
    return plain(*args)


def solution(mesh):
    return jax.shard_map(
        functools.partial(per_device, mesh.shape["rep"], mesh.shape["tp"]),
        mesh=mesh,
        in_specs=(
            P("rep", None),
            P(("rep", "tp"), None),
            P(("rep", "tp"), None),
            P(("rep", "tp"), None),
            P("rep", None, "tp"),
            P("rep", None, "tp"),
            P("rep", None),
            P("rep", None, None),
        ),
        out_specs=(P("rep", "tp"), P(None, "rep", "tp")),
        check_vma=False,
    )
```

```python
import functools

import jax
import jax.numpy as jnp
from jax import lax
from jax.experimental import pallas as pl
from jax.experimental.pallas import tpu as pltpu
from jax.sharding import PartitionSpec as P

HEADS = 64
KV_HEADS = 8
HEAD_DIM = 128
SEQS = 2
NEW = 256
TOK = 512
MAXLEN = 2048
ROPE_THETA = 500000.0
KEY_BLOCK = 512
VMEM_LIMIT = 56 * 1024 * 1024
BF = jnp.bfloat16

HEAD_CHUNKS = (0, 3, 3, 2)
SPLIT = ()
OWN_ORDER = (0, 1, 2, 3)


def plain_rotate(vectors, positions):
    half_dim = HEAD_DIM // 2
    frequency = ROPE_THETA ** (-2.0 * jnp.arange(half_dim, dtype=jnp.float32) / HEAD_DIM)
    angles = positions.astype(jnp.float32)[:, None] * frequency[None, :]
    cosine_part = jnp.cos(angles)[:, None, :]
    sine_part = jnp.sin(angles)[:, None, :]
    first_half = vectors[..., :half_dim]
    second_half = vectors[..., half_dim:]
    return jnp.concatenate(
        [
            first_half * cosine_part - second_half * sine_part,
            second_half * cosine_part + first_half * sine_part,
        ],
        axis=-1,
    )


def plain(
    tokens, query_weight, key_weight, value_weight, cache_keys, cache_values, lengths, page_table
):
    weights = (
        query_weight.astype(jnp.bfloat16),
        key_weight.astype(jnp.bfloat16),
        value_weight.astype(jnp.bfloat16),
    )
    slabs = (
        lax.all_to_all(weights[0], "tp", split_axis=1, concat_axis=0, tiled=True),
        lax.all_to_all(weights[1], "tp", split_axis=1, concat_axis=0, tiled=True),
        lax.all_to_all(weights[2], "tp", split_axis=1, concat_axis=0, tiled=True),
    )
    pieces = (
        lax.all_gather(slabs[0], "rep", axis=0, tiled=True),
        lax.all_gather(slabs[1], "rep", axis=0, tiled=True),
        lax.all_gather(slabs[2], "rep", axis=0, tiled=True),
    )
    raw_query, raw_key, raw_value = tuple(
        (jnp.dot(tokens, piece, preferred_element_type=jnp.float32) for piece in pieces)
    )
    kv_local = raw_key.shape[1] // HEAD_DIM
    group_size = HEADS // KV_HEADS
    scale = 1.0 / HEAD_DIM**0.5
    seq_lengths = lengths[0]
    positions = (seq_lengths[:, None] + jnp.arange(NEW, dtype=jnp.int32)[None, :]).reshape(TOK)
    queries = plain_rotate(raw_query.reshape(TOK, kv_local * group_size, HEAD_DIM), positions).astype(
        jnp.bfloat16
    )
    new_keys = plain_rotate(raw_key.reshape(TOK, kv_local, HEAD_DIM), positions).astype(jnp.bfloat16)
    new_values = raw_value.astype(jnp.bfloat16).reshape(TOK, kv_local, HEAD_DIM)

    def one_sequence(inner):
        seq_queries, seq_keys, seq_values, page_rows, length = inner
        old_keys = cache_keys[page_rows].reshape(MAXLEN, kv_local, HEAD_DIM)
        old_values = cache_values[page_rows].reshape(MAXLEN, kv_local, HEAD_DIM)
        all_keys = jnp.concatenate([old_keys, seq_keys], axis=0)
        all_values = jnp.concatenate([old_values, seq_values], axis=0)
        grouped = seq_queries.reshape(NEW, kv_local, group_size, HEAD_DIM)
        scores = (
            jnp.einsum("nkgd,mkd->kgnm", grouped, all_keys, preferred_element_type=jnp.float32)
            * scale
        )
        key_index = jnp.arange(MAXLEN + NEW, dtype=jnp.int32)[None, :]
        query_index = jnp.arange(NEW, dtype=jnp.int32)[:, None]
        visible = jnp.where(
            key_index < MAXLEN, key_index < length, key_index - MAXLEN <= query_index
        )
        scores = jnp.where(visible[None, None], scores, -1e30)
        maxima = jnp.max(scores, axis=-1, keepdims=True)
        expons = jnp.exp(scores - maxima)
        probs = (expons / jnp.sum(expons, axis=-1, keepdims=True)).astype(jnp.bfloat16)
        output = jnp.einsum("kgnm,mkd->nkgd", probs, all_values, preferred_element_type=jnp.float32)
        return output.astype(jnp.bfloat16).reshape(NEW, kv_local * group_size * HEAD_DIM)

    attended = lax.map(
        one_sequence,
        (
            queries.reshape(SEQS, NEW, kv_local * group_size, HEAD_DIM),
            new_keys.reshape(SEQS, NEW, kv_local, HEAD_DIM),
            new_values.reshape(SEQS, NEW, kv_local, HEAD_DIM),
            page_table[0],
            seq_lengths,
        ),
    )
    new_cache = jnp.stack(
        [new_keys.reshape(TOK, kv_local * HEAD_DIM), new_values.reshape(TOK, kv_local * HEAD_DIM)]
    )
    return (attended.reshape(TOK, kv_local * group_size * HEAD_DIM), new_cache)


def rotate(v, cos, sin):
    half = HEAD_DIM // 2
    swapped = jnp.concatenate([v[:, half:], v[:, :half]], axis=1)
    return v * cos + swapped * sin


def pack_kernel(jobs, n_recv, starts_ref, *refs):
    weights, received = refs[:3], refs[3 : 3 + n_recv]
    outs = refs[3 + n_recv : 3 + n_recv + len(jobs)]
    buf, sems = refs[-2:]
    flat, at = [], 0
    for out, pieces in zip(outs, jobs):
        for row, col, width, source, begin in pieces:
            if source >= 3:
                continue
            src = weights[source].at[:, pl.ds(pl.multiple_of(starts_ref[begin], 128), width)]
            copy = pltpu.make_async_copy(src, buf.at[:, pl.ds(at, width)], sems.at[len(flat)])
            copy.start()
            flat.append((copy, out, row, col, width, at))
            at += width
    rows = buf.shape[0]
    for out, pieces in zip(outs, jobs):
        for row, col, width, source, begin in pieces:
            if source >= 3:
                out[row : row + rows, col : col + width] = received[source - 3][:, begin : begin + width]
    for copy, out, row, col, width, at in flat:
        copy.wait()
        out[row : row + rows, col : col + width] = buf[:, at : at + width].astype(BF)


def pack(jobs, shapes, starts, weights, received):
    n = sum(1 for pieces in jobs for piece in pieces if piece[3] < 3)
    total = sum(piece[2] for pieces in jobs for piece in pieces if piece[3] < 3)
    rows = weights[0].shape[0]
    return pl.pallas_call(
        functools.partial(pack_kernel, jobs, len(received)),
        out_shape=[jax.ShapeDtypeStruct(shape, BF) for shape in shapes],
        grid_spec=pltpu.PrefetchScalarGridSpec(
            num_scalar_prefetch=1,
            grid=(1,),
            in_specs=[pl.BlockSpec(memory_space=pl.ANY)] * 3
            + [pl.BlockSpec(a.shape, lambda i, _: (0, 0)) for a in received],
            out_specs=[pl.BlockSpec(shape, lambda i, _: (0, 0)) for shape in shapes],
            scratch_shapes=[pltpu.VMEM((rows, total), jnp.float32), pltpu.SemaphoreType.DMA((n,))],
        ),
        compiler_params=pltpu.CompilerParams(vmem_limit_bytes=VMEM_LIMIT),
        cost_estimate=pl.CostEstimate(flops=1000000, bytes_accessed=rows * total * 6, transcendentals=0),
    )(starts, *weights, *received)


def move_kernel(jobs, *refs):
    n_in = 1 + max(job[0] for job in jobs)
    ins, outs, sems = refs[:n_in], refs[n_in:-1], refs[-1]
    copies = []
    for k, (source, first, rows, target, to) in enumerate(jobs):
        copies.append(
            pltpu.make_async_copy(
                ins[source].at[pl.ds(first, rows)], outs[target].at[pl.ds(to, rows)], sems.at[k]
            )
        )
        copies[-1].start()
    for copy in copies:
        copy.wait()


def move(jobs, arrays, shapes):
    return pl.pallas_call(
        functools.partial(move_kernel, jobs),
        out_shape=[jax.ShapeDtypeStruct(shape, BF) for shape in shapes],
        in_specs=[pl.BlockSpec(memory_space=pl.ANY)] * len(arrays),
        out_specs=[pl.BlockSpec(memory_space=pltpu.VMEM)] * len(shapes),
        scratch_shapes=[pltpu.SemaphoreType.DMA((len(jobs),))],
        compiler_params=pltpu.CompilerParams(vmem_limit_bytes=16 * 1024 * 1024),
        cost_estimate=pl.CostEstimate(
            flops=1000000, bytes_accessed=sum(4 * a * b for a, b in shapes), transcendentals=0
        ),
    )(*arrays)


def lanes(x):
    return [x[:, i * 128 : (i + 1) * 128] for i in range(x.shape[1] // 128)]


def spread(column):
    return jnp.broadcast_to(column, (column.shape[0], 128))


def pages_kernel(core_ref, table_ref, ck_ref, cv_ref, mine_ref, theirs_ref, sems):
    seqs, pages = table_ref.shape
    size = ck_ref.shape[1]
    copies = []
    for k, ref in enumerate((ck_ref, cv_ref)):
        for s in range(seqs):
            for p in range(pages):
                for h, out in ((core_ref[0], mine_ref), (1 - core_ref[0], theirs_ref)):
                    src = ref.at[table_ref[s, p], :, pl.ds(pl.multiple_of(h * HEAD_DIM, HEAD_DIM), HEAD_DIM)]
                    copy = pltpu.make_async_copy(src, out.at[k, s, pl.ds(p * size, size)], sems.at[len(copies)])
                    copy.start()
                    copies.append(copy)
    for copy in copies:
        copy.wait()


def chunk_kernel(
    shard, places, heads, with_kv, block, base, n_out, len_ref, order_ref, cos_ref, sin_ref,
    their_tok, my_tok, their_old, my_old, *refs
):
    if not with_kv:
        fresh_ref, refs = refs[0], refs[1:]
    weights, refs = refs[: len(places)], refs[len(places) :]
    out_refs, refs = refs[:n_out], refs[n_out:]
    if with_kv:
        fresh_ref, refs = refs[0], refs[1:]
    tok_ref, w_ref, old_ref, q_ref, e_ref, m_ref, l_ref, top_ref, acc_ref, sems, w_sems = refs
    step = pl.program_id(0)
    steps = pl.num_programs(0)
    i = step + base
    slot = step % 2
    new = tok_ref.shape[1]
    length = len_ref[i]
    blocks = (length + block - 1) // block
    factor = (1.0 / HEAD_DIM**0.5) * 1.4426950408889634
    nt = (((1,), (1,)), ((), ()))
    seqs = their_old.shape[1]

    def inputs(tok, old, seq, slot):
        return [
            pltpu.make_async_copy(tok.at[pl.ds(seq * new, new)], tok_ref.at[slot], sems.at[slot, 0]),
            pltpu.make_async_copy(old.at[0, seq], old_ref.at[slot, 0], sems.at[slot, 1]),
            pltpu.make_async_copy(old.at[1, seq], old_ref.at[slot, 1], sems.at[slot, 2]),
        ]

    def fetch(seq, slot):
        @pl.when(seq < seqs)
        def _():
            for copy in inputs(their_tok, their_old, seq, slot):
                copy.start()

        @pl.when(seq >= seqs)
        def _():
            for copy in inputs(my_tok, my_old, seq - seqs, slot):
                copy.start()

    copies = []
    for (entry, col), ref in zip(places, weights):
        for j in range(ref.shape[0] // shard):
            to = pl.multiple_of(order_ref[entry + j] * shard, shard)
            copies.append(
                pltpu.make_async_copy(
                    ref.at[pl.ds(j * shard, shard), pl.ds(col, w_ref.shape[1])],
                    w_ref.at[pl.ds(to, shard)],
                    w_sems.at[len(copies)],
                )
            )

    @pl.when(step == 0)
    def _():
        fetch(i, slot)
        for copy in copies:
            copy.start()

    @pl.when(step + 1 < steps)
    def _():
        fetch(i + 1, 1 - slot)

    for copy in inputs(my_tok, my_old, 0, slot):
        copy.wait()

    @pl.when(step == 0)
    def _():
        for copy in copies:
            copy.wait()

    raw = jnp.dot(tok_ref[slot], w_ref[...], preferred_element_type=jnp.float32)
    raw = [raw[:, h * HEAD_DIM : (h + 1) * HEAD_DIM] for h in range(raw.shape[1] // HEAD_DIM)]
    if with_kv:
        fresh_ref[0] = rotate(raw[0], cos_ref[...], sin_ref[...]).astype(BF)
        fresh_ref[1] = raw[1].astype(BF)
        raw = raw[2:]
    if heads == 0:
        half = steps // 2

        def write_new(out_ref):
            for k in range(2):
                out_ref[:, k * HEAD_DIM : (k + 1) * HEAD_DIM] = fresh_ref[k]

        pl.when(step < half)(lambda: write_new(out_refs[0]))
        pl.when(step >= half)(lambda: write_new(out_refs[1]))
        return
    for h in range(heads):
        q_ref[h * new : (h + 1) * new, :] = rotate(raw[h], cos_ref[...], sin_ref[...]).astype(BF)

    s = lax.dot_general(q_ref[...], fresh_ref[0], nt, preferred_element_type=jnp.float32)
    row = lax.broadcasted_iota(jnp.int32, s.shape, 0) % new
    col = lax.broadcasted_iota(jnp.int32, s.shape, 1)
    parts = lanes(jnp.where(col <= row, s, -1e30))
    m = functools.reduce(jnp.maximum, parts)
    es = [jnp.exp2((c - m) * factor) for c in parts]
    for j, e in enumerate(es):
        e_ref[0, :, j * 128 : (j + 1) * 128] = e
    m_ref[0] = m
    l_ref[...] = sum(es)

    @pl.loop(0, blocks)
    def _(b):
        start = pl.multiple_of(b * block, block)
        s = lax.dot_general(q_ref[...], old_ref[slot, 0, pl.ds(start, block), :], nt, preferred_element_type=jnp.float32)
        at = lax.broadcasted_iota(jnp.int32, s.shape, 1)
        parts = lanes(jnp.where(at < length - start, s, -1e30))
        before = m_ref[b]
        m = functools.reduce(jnp.maximum, parts, before)
        es = [jnp.exp2((c - m) * factor) for c in parts]
        for j, e in enumerate(es):
            e_ref[b + 1, :, j * 128 : (j + 1) * 128] = e
        m_ref[b + 1] = m
        l_ref[...] = l_ref[...] * jnp.exp2((before - m) * factor) + sum(es)

    last = m_ref[blocks]
    top = spread(jnp.max(last, axis=1, keepdims=True))
    total = jnp.sum(l_ref[...] * jnp.exp2((last - top) * factor), axis=1, keepdims=True)
    top_ref[...] = top
    inverse = spread(1.0 / total)
    l_ref[...] = inverse

    def probs(slot, n):
        scale = jnp.exp2((m_ref[slot] - top_ref[...]) * factor) * l_ref[...]
        return jnp.concatenate(
            [(e_ref[slot, :, j * 128 : (j + 1) * 128] * scale).astype(BF) for j in range(n)], axis=1
        )

    acc_ref[...] = jnp.dot(probs(0, new // 128), fresh_ref[1], preferred_element_type=jnp.float32)

    @pl.loop(0, blocks)
    def _(b):
        start = pl.multiple_of(b * block, block)
        acc_ref[...] += jnp.dot(
            probs(b + 1, block // 128), old_ref[slot, 1, pl.ds(start, block), :], preferred_element_type=jnp.float32
        )

    def write(out_ref):
        if with_kv:
            for k in range(2):
                cols = slice((heads + k) * HEAD_DIM, (heads + k + 1) * HEAD_DIM)
                out_ref[:, cols] = fresh_ref[k]
        for h in range(heads):
            out_ref[:, h * HEAD_DIM : (h + 1) * HEAD_DIM] = acc_ref[h * new : (h + 1) * new, :].astype(BF)

    if n_out == 1:
        write(out_refs[0])
    else:
        half = pl.num_programs(0) // 2
        pl.when(step < half)(lambda: write(out_refs[0]))
        pl.when(step >= half)(lambda: write(out_refs[1]))


def by_core(R, T, tokens, query_weight, key_weight, value_weight, cache_keys, cache_values, lengths, page_table):
    tok_rows, depth = tokens.shape
    shard = query_weight.shape[0]
    seqs = lengths.shape[1]
    new = tok_rows // seqs
    q_local = query_weight.shape[1] // T
    q_core = q_local // 2
    kv_width = key_weight.shape[1] // T
    r, z = lax.axis_index("rep"), lax.axis_index("tp")
    core = r % 2
    max_len = cache_keys.shape[1] * page_table.shape[2]

    def xor(a, bit):
        return lax.ppermute(a, "rep", [(i, i ^ bit) for i in range(R)])

    head_chunks = HEAD_CHUNKS
    widths = [(n + 2 * (c == 0)) * HEAD_DIM for c, n in enumerate(head_chunks)]
    firsts = [sum(widths[:c]) for c in range(len(widths))]
    own_firsts, col = {}, 0
    for c in OWN_ORDER:
        own_firsts[c] = col
        col += widths[c]
    whole = sum(widths)
    n_chunks = len(widths)

    starts = []
    for s in range(T):
        target = (z + s) % T
        for h in (core, 1 - core):
            starts += [target * q_local + h * q_core, target * kv_width + h * HEAD_DIM, target * kv_width + h * HEAD_DIM]
    for s in range(T):
        target = (z + s) % T
        for h in (core, 1 - core):
            base = target * q_local + h * q_core
            starts += [base + firsts[c] - 2 * HEAD_DIM if c else base for c in range(n_chunks)]
    starts = jnp.stack(starts).astype(jnp.int32)
    weights = (query_weight, key_weight, value_weight)

    def pieces(s, other, c, row, col):
        base, q_base = 3 * (2 * s + other), 6 * T + n_chunks * (2 * s + other)
        if c:
            return [(row, col, widths[c], 0, q_base + c)]
        return [
            (row, col, HEAD_DIM, 1, base + 1),
            (row, col + HEAD_DIM, HEAD_DIM, 2, base + 2),
        ] + ([(row, col + 2 * HEAD_DIM, widths[0] - 2 * HEAD_DIM, 0, q_base)] if head_chunks[0] else [])

    def all_chunks(s, other, row, col):
        return [p for c in range(n_chunks) for p in pieces(s, other, c, row, col + own_firsts[c])]

    def their_half(chunks):
        job, col, place = [], 0, {}
        for c in chunks:
            for s in range(1, T):
                job += pieces(s, 1, c, 0, col)
                place[s, c] = col
                col += widths[c]
        return pack([job], [(shard, col)], starts, weights, [])[0], place

    def to_send(got, place):
        jobs, shapes = [], []
        for s, c in place:
            jobs.append(pieces(s, 0, c, 0, 0) + [(shard, 0, widths[c], 3, place[s, c])])
            shapes.append((2 * shard, widths[c]))
        return dict(zip(place, pack(jobs, shapes, starts, weights, [got])))

    send_b, place_b = their_half([0])
    got_b = xor(send_b, 1)
    own_mine = pack([all_chunks(0, 0, 0, 0)], [(shard, whole)], starts, weights, [])[0]
    ready = to_send(got_b, place_b)
    send_a = pack([all_chunks(0, 1, 0, 0)], [(shard, whole)], starts, weights, [])[0]
    own_other = xor(send_a, 1)
    send_c, place_c = their_half(range(1, n_chunks))
    got_c = xor(send_c, 1)
    ready.update(to_send(got_c, place_c))

    def over_tp(c):
        got = []
        for s in range(1, T):
            got.append(lax.ppermute(ready[s, c], "tp", [(t, (t + s) % T) for t in range(T)]))
        rows = got[0].shape[0]
        jobs = [(k, 0, rows, 0, k * rows) for k in range(T - 1)]
        return move(jobs, got, [((T - 1) * rows, widths[c])])[0]

    def gather(piece):
        by_x, by_y = xor(piece, 2), xor(piece, 4)
        n = piece.shape[0] // 2
        jobs = [(0, 0, n, 0, 0), (1, n, n, 1, 0)]
        low, high = move(jobs, [by_y, by_x], [(n, piece.shape[1])] * 2)
        far = [(6, 0, xor(low, 2)), (6, n, xor(high, 4))]
        return [(0, 0, piece), (2, 0, by_x), (4, 0, by_y), *far]

    by_x, by_y = xor(own_mine, 2), xor(own_mine, 4)
    other_x, other_y = xor(own_other, 2), xor(own_other, 4)
    own_all = [
        (0, 0, own_mine), (0, shard, own_other), (2, 0, by_x), (2, shard, other_x), (4, 0, by_y),
        (4, shard, other_y), (6, 0, xor(by_y, 2)), (6, shard, xor(other_x, 4)),
    ]
    rest_all = [gather(over_tp(c)) for c in range(n_chunks)]

    their_tokens = xor(tokens, 1)
    seq_lengths = jnp.concatenate([xor(lengths, 1)[0], lengths[0]])
    old_shape = (2, seqs, max_len, HEAD_DIM)
    call = pl.pallas_call(
        pages_kernel,
        out_shape=[jax.ShapeDtypeStruct(old_shape, BF)] * 2,
        grid_spec=pltpu.PrefetchScalarGridSpec(
            num_scalar_prefetch=2,
            grid=(1,),
            in_specs=[pl.BlockSpec(memory_space=pl.ANY)] * 2,
            out_specs=[pl.BlockSpec(old_shape, lambda i, *_: (0, 0, 0, 0))] * 2,
            scratch_shapes=[pltpu.SemaphoreType.DMA((4 * seqs * page_table.shape[2],))],
        ),
        compiler_params=pltpu.CompilerParams(vmem_limit_bytes=VMEM_LIMIT),
        cost_estimate=pl.CostEstimate(flops=1000000, bytes_accessed=8000000, transcendentals=0),
        name="old",
    )
    my_old, for_them = call(core[None].astype(jnp.int32), page_table[0], cache_keys, cache_values)
    their_old = xor(for_them, 1)

    order, place = [], {}
    for shifts in ([0], list(range(1, T))):
        for d in range(0, R, 2):
            place[d, shifts[0]] = len(order)
            order += [(r ^ (d + e)) * T + (z - s) % T for s in shifts for e in range(2)]
    order = jnp.stack(order).astype(jnp.int32)
    rows_all = 2 * tok_rows
    params = pltpu.CompilerParams(vmem_limit_bytes=VMEM_LIMIT)

    half = HEAD_DIM // 2
    frequency = ROPE_THETA ** (-2.0 * jnp.arange(half, dtype=jnp.float32) / HEAD_DIM)
    positions = (seq_lengths[:, None] + jnp.arange(new, dtype=jnp.int32)[None, :]).reshape(rows_all)
    angles = positions.astype(jnp.float32)[:, None] * frequency[None, :]
    cos, sin = jnp.cos(angles), jnp.sin(angles)
    cos, sin = jnp.concatenate([cos, cos], axis=1), jnp.concatenate([-sin, sin], axis=1)

    def attend(c, fresh, group=None):
        n = head_chunks[c]
        width = n * HEAD_DIM
        with_kv = c == 0
        base = seqs * (group or 0)
        count = seqs if group is not None else 2 * seqs
        n_out = count // seqs
        block = KEY_BLOCK
        slots = max_len // block + 1
        m = max(n, 1) * new
        arrays, places = [], []
        for s, first, parts in ((0, own_firsts[c], own_all), (1, 0, rest_all[c])):
            for d, o, a in parts:
                arrays.append(a)
                places.append((place[d, s] + o // shard, first))
        row = lambda i, *_: (i + base, 0)
        out_width = width + 2 * HEAD_DIM * with_kv
        out_shape = [jax.ShapeDtypeStruct((tok_rows, out_width), BF)] * n_out
        if n_out == 1:
            out_specs = [pl.BlockSpec((new, out_width), lambda i, *_: (i, 0))]
        else:
            out_specs = [
                pl.BlockSpec((new, out_width), lambda i, *_: (jnp.minimum(i, seqs - 1), 0)),
                pl.BlockSpec((new, out_width), lambda i, *_: (jnp.maximum(i - seqs, 0), 0)),
            ]
        fresh_spec = pl.BlockSpec((2, new, HEAD_DIM), lambda i, *_: (0, i + base, 0))
        if with_kv:
            out_shape.append(jax.ShapeDtypeStruct((2, rows_all, HEAD_DIM), BF))
            out_specs.append(fresh_spec)
        anywhere = pl.BlockSpec(memory_space=pl.ANY)
        call = pl.pallas_call(
            functools.partial(chunk_kernel, shard, places, n, with_kv, block, base, n_out),
            out_shape=out_shape,
            grid_spec=pltpu.PrefetchScalarGridSpec(
                num_scalar_prefetch=2,
                grid=(count,),
                in_specs=[
                    pl.BlockSpec((new, HEAD_DIM), row),
                    pl.BlockSpec((new, HEAD_DIM), row),
                    *[anywhere] * 4,
                    *([] if with_kv else [fresh_spec]),
                    *[anywhere] * len(arrays),
                ],
                out_specs=out_specs,
                scratch_shapes=[
                    pltpu.VMEM((2, new, depth), BF),
                    pltpu.VMEM((depth, widths[c]), BF),
                    pltpu.VMEM((2, 2, max_len, HEAD_DIM), BF),
                    pltpu.VMEM((m, HEAD_DIM), BF),
                    pltpu.VMEM((slots, m, block), jnp.float32),
                    pltpu.VMEM((slots, m, 128), jnp.float32),
                    pltpu.VMEM((m, 128), jnp.float32),
                    pltpu.VMEM((m, 128), jnp.float32),
                    pltpu.VMEM((m, 128), jnp.float32),
                    pltpu.SemaphoreType.DMA((2, 3)),
                    pltpu.SemaphoreType.DMA((depth // shard,)),
                ],
            ),
            compiler_params=params,
            cost_estimate=pl.CostEstimate(
                flops=count * new * width * 2 * (depth + 2 * (max_len + new)),
                bytes_accessed=(count * new + width) * depth * 2,
                transcendentals=count * new * n * (max_len + new),
            ),
        )
        extra = () if with_kv else (fresh,)
        return call(
            seq_lengths, order, cos, sin, their_tokens, tokens, their_old, my_old, *extra, *arrays
        )

    out, at, fresh = jnp.zeros((tok_rows, q_local), BF), 0, None
    for c in range(n_chunks):
        if c in SPLIT:
            (theirs,), (mine,) = attend(c, fresh, 0), attend(c, fresh, 1)
        else:
            theirs, mine, *rest = attend(c, fresh)
        theirs = xor(theirs, 1)
        width = head_chunks[c] * HEAD_DIM
        if c == 0:
            fresh = rest[0]
            parts = []
            for k in range(2):
                cols = slice(width + k * HEAD_DIM, width + (k + 1) * HEAD_DIM)
                pair = (mine[:, cols], theirs[:, cols])
                parts.append(
                    jnp.concatenate([jnp.where(core == 0, *pair), jnp.where(core == 0, *pair[::-1])], axis=1)
                )
            new_cache = jnp.stack(parts)
        if not width:
            continue
        out = lax.dynamic_update_slice(out, mine[:, :width], (0, core * q_core + at))
        out = lax.dynamic_update_slice(out, theirs[:, :width], (0, (1 - core) * q_core + at))
        at += width
    return out, new_cache


def per_device(R, T, *args):
    _, query_weight, key_weight = args[:3]
    heads = query_weight.shape[1] // T // HEAD_DIM
    kv = key_weight.shape[1] // T // HEAD_DIM
    if R == 8 and kv == 2 and heads == 16:
        return by_core(R, T, *args)
    return plain(*args)


def solution(mesh):
    return jax.shard_map(
        functools.partial(per_device, mesh.shape["rep"], mesh.shape["tp"]),
        mesh=mesh,
        in_specs=(
            P("rep", None),
            P(("rep", "tp"), None),
            P(("rep", "tp"), None),
            P(("rep", "tp"), None),
            P("rep", None, "tp"),
            P("rep", None, "tp"),
            P("rep", None),
            P("rep", None, None),
        ),
        out_specs=(P("rep", "tp"), P(None, "rep", "tp")),
        check_vma=False,
    )
```

```python
import functools

import jax
import jax.numpy as jnp
from jax import lax
from jax.experimental import pallas as pl
from jax.experimental.pallas import tpu as pltpu
from jax.sharding import PartitionSpec as P

HEADS = 64
KV_HEADS = 8
HEAD_DIM = 128
SEQS = 2
NEW = 256
TOK = 512
MAXLEN = 2048
ROPE_THETA = 500000.0
KEY_BLOCK = 512
VMEM_LIMIT = 56 * 1024 * 1024
BF = jnp.bfloat16

HEAD_CHUNKS = (0, 4, 4)
SPLIT = (1, 2)
OWN_ORDER = (0, 1, 2)


def plain_rotate(vectors, positions):
    half_dim = HEAD_DIM // 2
    frequency = ROPE_THETA ** (-2.0 * jnp.arange(half_dim, dtype=jnp.float32) / HEAD_DIM)
    angles = positions.astype(jnp.float32)[:, None] * frequency[None, :]
    cosine_part = jnp.cos(angles)[:, None, :]
    sine_part = jnp.sin(angles)[:, None, :]
    first_half = vectors[..., :half_dim]
    second_half = vectors[..., half_dim:]
    return jnp.concatenate(
        [
            first_half * cosine_part - second_half * sine_part,
            second_half * cosine_part + first_half * sine_part,
        ],
        axis=-1,
    )


def plain(
    tokens, query_weight, key_weight, value_weight, cache_keys, cache_values, lengths, page_table
):
    weights = (
        query_weight.astype(jnp.bfloat16),
        key_weight.astype(jnp.bfloat16),
        value_weight.astype(jnp.bfloat16),
    )
    slabs = (
        lax.all_to_all(weights[0], "tp", split_axis=1, concat_axis=0, tiled=True),
        lax.all_to_all(weights[1], "tp", split_axis=1, concat_axis=0, tiled=True),
        lax.all_to_all(weights[2], "tp", split_axis=1, concat_axis=0, tiled=True),
    )
    pieces = (
        lax.all_gather(slabs[0], "rep", axis=0, tiled=True),
        lax.all_gather(slabs[1], "rep", axis=0, tiled=True),
        lax.all_gather(slabs[2], "rep", axis=0, tiled=True),
    )
    raw_query, raw_key, raw_value = tuple(
        (jnp.dot(tokens, piece, preferred_element_type=jnp.float32) for piece in pieces)
    )
    kv_local = raw_key.shape[1] // HEAD_DIM
    group_size = HEADS // KV_HEADS
    scale = 1.0 / HEAD_DIM**0.5
    seq_lengths = lengths[0]
    positions = (seq_lengths[:, None] + jnp.arange(NEW, dtype=jnp.int32)[None, :]).reshape(TOK)
    queries = plain_rotate(raw_query.reshape(TOK, kv_local * group_size, HEAD_DIM), positions).astype(
        jnp.bfloat16
    )
    new_keys = plain_rotate(raw_key.reshape(TOK, kv_local, HEAD_DIM), positions).astype(jnp.bfloat16)
    new_values = raw_value.astype(jnp.bfloat16).reshape(TOK, kv_local, HEAD_DIM)

    def one_sequence(inner):
        seq_queries, seq_keys, seq_values, page_rows, length = inner
        old_keys = cache_keys[page_rows].reshape(MAXLEN, kv_local, HEAD_DIM)
        old_values = cache_values[page_rows].reshape(MAXLEN, kv_local, HEAD_DIM)
        all_keys = jnp.concatenate([old_keys, seq_keys], axis=0)
        all_values = jnp.concatenate([old_values, seq_values], axis=0)
        grouped = seq_queries.reshape(NEW, kv_local, group_size, HEAD_DIM)
        scores = (
            jnp.einsum("nkgd,mkd->kgnm", grouped, all_keys, preferred_element_type=jnp.float32)
            * scale
        )
        key_index = jnp.arange(MAXLEN + NEW, dtype=jnp.int32)[None, :]
        query_index = jnp.arange(NEW, dtype=jnp.int32)[:, None]
        visible = jnp.where(
            key_index < MAXLEN, key_index < length, key_index - MAXLEN <= query_index
        )
        scores = jnp.where(visible[None, None], scores, -1e30)
        maxima = jnp.max(scores, axis=-1, keepdims=True)
        expons = jnp.exp(scores - maxima)
        probs = (expons / jnp.sum(expons, axis=-1, keepdims=True)).astype(jnp.bfloat16)
        output = jnp.einsum("kgnm,mkd->nkgd", probs, all_values, preferred_element_type=jnp.float32)
        return output.astype(jnp.bfloat16).reshape(NEW, kv_local * group_size * HEAD_DIM)

    attended = lax.map(
        one_sequence,
        (
            queries.reshape(SEQS, NEW, kv_local * group_size, HEAD_DIM),
            new_keys.reshape(SEQS, NEW, kv_local, HEAD_DIM),
            new_values.reshape(SEQS, NEW, kv_local, HEAD_DIM),
            page_table[0],
            seq_lengths,
        ),
    )
    new_cache = jnp.stack(
        [new_keys.reshape(TOK, kv_local * HEAD_DIM), new_values.reshape(TOK, kv_local * HEAD_DIM)]
    )
    return (attended.reshape(TOK, kv_local * group_size * HEAD_DIM), new_cache)


def rotate(v, cos, sin):
    half = HEAD_DIM // 2
    swapped = jnp.concatenate([v[:, half:], v[:, :half]], axis=1)
    return v * cos + swapped * sin


def pack_kernel(jobs, n_recv, starts_ref, *refs):
    weights, received = refs[:3], refs[3 : 3 + n_recv]
    outs = refs[3 + n_recv : 3 + n_recv + len(jobs)]
    buf, sems = refs[-2:]
    flat, at = [], 0
    for out, pieces in zip(outs, jobs):
        for row, col, width, source, begin in pieces:
            if source >= 3:
                continue
            src = weights[source].at[:, pl.ds(pl.multiple_of(starts_ref[begin], 128), width)]
            copy = pltpu.make_async_copy(src, buf.at[:, pl.ds(at, width)], sems.at[len(flat)])
            copy.start()
            flat.append((copy, out, row, col, width, at))
            at += width
    rows = buf.shape[0]
    for out, pieces in zip(outs, jobs):
        for row, col, width, source, begin in pieces:
            if source >= 3:
                out[row : row + rows, col : col + width] = received[source - 3][:, begin : begin + width]
    for copy, out, row, col, width, at in flat:
        copy.wait()
        out[row : row + rows, col : col + width] = buf[:, at : at + width].astype(BF)


def pack(jobs, shapes, starts, weights, received):
    n = sum(1 for pieces in jobs for piece in pieces if piece[3] < 3)
    total = sum(piece[2] for pieces in jobs for piece in pieces if piece[3] < 3)
    rows = weights[0].shape[0]
    return pl.pallas_call(
        functools.partial(pack_kernel, jobs, len(received)),
        out_shape=[jax.ShapeDtypeStruct(shape, BF) for shape in shapes],
        grid_spec=pltpu.PrefetchScalarGridSpec(
            num_scalar_prefetch=1,
            grid=(1,),
            in_specs=[pl.BlockSpec(memory_space=pl.ANY)] * 3
            + [pl.BlockSpec(a.shape, lambda i, _: (0, 0)) for a in received],
            out_specs=[pl.BlockSpec(shape, lambda i, _: (0, 0)) for shape in shapes],
            scratch_shapes=[pltpu.VMEM((rows, total), jnp.float32), pltpu.SemaphoreType.DMA((n,))],
        ),
        compiler_params=pltpu.CompilerParams(vmem_limit_bytes=VMEM_LIMIT),
        cost_estimate=pl.CostEstimate(flops=1000000, bytes_accessed=rows * total * 6, transcendentals=0),
    )(starts, *weights, *received)


def move_kernel(jobs, *refs):
    n_in = 1 + max(job[0] for job in jobs)
    ins, outs, sems = refs[:n_in], refs[n_in:-1], refs[-1]
    copies = []
    for k, (source, first, rows, target, to) in enumerate(jobs):
        copies.append(
            pltpu.make_async_copy(
                ins[source].at[pl.ds(first, rows)], outs[target].at[pl.ds(to, rows)], sems.at[k]
            )
        )
        copies[-1].start()
    for copy in copies:
        copy.wait()


def move(jobs, arrays, shapes):
    return pl.pallas_call(
        functools.partial(move_kernel, jobs),
        out_shape=[jax.ShapeDtypeStruct(shape, BF) for shape in shapes],
        in_specs=[pl.BlockSpec(memory_space=pl.ANY)] * len(arrays),
        out_specs=[pl.BlockSpec(memory_space=pltpu.VMEM)] * len(shapes),
        scratch_shapes=[pltpu.SemaphoreType.DMA((len(jobs),))],
        compiler_params=pltpu.CompilerParams(vmem_limit_bytes=16 * 1024 * 1024),
        cost_estimate=pl.CostEstimate(
            flops=1000000, bytes_accessed=sum(4 * a * b for a, b in shapes), transcendentals=0
        ),
    )(*arrays)


def lanes(x):
    return [x[:, i * 128 : (i + 1) * 128] for i in range(x.shape[1] // 128)]


def spread(column):
    return jnp.broadcast_to(column, (column.shape[0], 128))


def pages_kernel(core_ref, table_ref, ck_ref, cv_ref, mine_ref, theirs_ref, sems):
    seqs, pages = table_ref.shape
    size = ck_ref.shape[1]
    copies = []
    for k, ref in enumerate((ck_ref, cv_ref)):
        for s in range(seqs):
            for p in range(pages):
                for h, out in ((core_ref[0], mine_ref), (1 - core_ref[0], theirs_ref)):
                    src = ref.at[table_ref[s, p], :, pl.ds(pl.multiple_of(h * HEAD_DIM, HEAD_DIM), HEAD_DIM)]
                    copy = pltpu.make_async_copy(src, out.at[k, s, pl.ds(p * size, size)], sems.at[len(copies)])
                    copy.start()
                    copies.append(copy)
    for copy in copies:
        copy.wait()


def chunk_kernel(
    shard, places, parts, stage, heads, with_kv, block, base, n_out, len_ref, order_ref, chip_ref, cos_ref, sin_ref,
    their_tok, my_tok, their_old, my_old, *refs
):
    if stage == "after":
        before_ref, refs = refs[0], refs[1:]
    if not with_kv and stage != "before":
        fresh_ref, refs = refs[0], refs[1:]
    weights, refs = refs[: len(places)], refs[len(places) :]
    out_refs, refs = refs[:n_out], refs[n_out:]
    if with_kv:
        fresh_ref, refs = refs[0], refs[1:]
    tok_ref, w_ref, old_ref, q_ref, e_ref, m_ref, l_ref, top_ref, acc_ref, sems, w_sems = refs
    step = pl.program_id(0)
    steps = pl.num_programs(0)
    i = step + base
    slot = step % 2
    new = tok_ref.shape[1]
    length = len_ref[i]
    blocks = (length + block - 1) // block
    factor = (1.0 / HEAD_DIM**0.5) * 1.4426950408889634
    nt = (((1,), (1,)), ((), ()))
    seqs = their_old.shape[1]
    chip = w_ref.shape[0] // len(parts)

    def inputs(tok, old, seq, slot):
        copies = []
        for j, part in enumerate(parts):
            cols = pl.ds(pl.multiple_of(chip_ref[part] * chip, chip), chip)
            src = tok.at[pl.ds(seq * new, new), cols]
            copies.append(
                pltpu.make_async_copy(src, tok_ref.at[slot, :, pl.ds(j * chip, chip)], sems.at[slot, 2 + j])
            )
        if stage != "before":
            for k in range(2):
                copies.append(pltpu.make_async_copy(old.at[k, seq], old_ref.at[slot, k], sems.at[slot, k]))
        return copies

    def fetch(seq, slot):
        @pl.when(seq < seqs)
        def _():
            for copy in inputs(their_tok, their_old, seq, slot):
                copy.start()

        @pl.when(seq >= seqs)
        def _():
            for copy in inputs(my_tok, my_old, seq - seqs, slot):
                copy.start()

    copies = []
    for (entry, col, part), ref in zip(places, weights):
        for j in range(ref.shape[0] // shard):
            to = pl.multiple_of(part * chip + order_ref[entry + j] * shard, shard)
            copies.append(
                pltpu.make_async_copy(
                    ref.at[pl.ds(j * shard, shard), pl.ds(col, w_ref.shape[1])],
                    w_ref.at[pl.ds(to, shard)],
                    w_sems.at[len(copies)],
                )
            )

    @pl.when(step == 0)
    def _():
        fetch(i, slot)
        for copy in copies:
            copy.start()

    @pl.when(step + 1 < steps)
    def _():
        fetch(i + 1, 1 - slot)

    for copy in inputs(my_tok, my_old, 0, slot):
        copy.wait()

    @pl.when(step == 0)
    def _():
        for copy in copies:
            copy.wait()

    raw = jnp.dot(tok_ref[slot], w_ref[...], preferred_element_type=jnp.float32)
    if stage == "before":
        out_refs[0][...] = raw
        return
    if stage == "after":
        raw = raw + before_ref[...]
    raw = [raw[:, h * HEAD_DIM : (h + 1) * HEAD_DIM] for h in range(raw.shape[1] // HEAD_DIM)]
    if with_kv:
        fresh_ref[0] = rotate(raw[0], cos_ref[...], sin_ref[...]).astype(BF)
        fresh_ref[1] = raw[1].astype(BF)
        raw = raw[2:]
    if heads == 0:
        half = steps // 2

        def write_new(out_ref):
            for k in range(2):
                out_ref[:, k * HEAD_DIM : (k + 1) * HEAD_DIM] = fresh_ref[k]

        pl.when(step < half)(lambda: write_new(out_refs[0]))
        pl.when(step >= half)(lambda: write_new(out_refs[1]))
        return
    for h in range(heads):
        q_ref[h * new : (h + 1) * new, :] = rotate(raw[h], cos_ref[...], sin_ref[...]).astype(BF)

    s = lax.dot_general(q_ref[...], fresh_ref[0], nt, preferred_element_type=jnp.float32)
    row = lax.broadcasted_iota(jnp.int32, s.shape, 0) % new
    col = lax.broadcasted_iota(jnp.int32, s.shape, 1)
    parts = lanes(jnp.where(col <= row, s, -1e30))
    m = functools.reduce(jnp.maximum, parts)
    es = [jnp.exp2((c - m) * factor) for c in parts]
    for j, e in enumerate(es):
        e_ref[0, :, j * 128 : (j + 1) * 128] = e
    m_ref[0] = m
    l_ref[...] = sum(es)

    @pl.loop(0, blocks)
    def _(b):
        start = pl.multiple_of(b * block, block)
        s = lax.dot_general(q_ref[...], old_ref[slot, 0, pl.ds(start, block), :], nt, preferred_element_type=jnp.float32)
        at = lax.broadcasted_iota(jnp.int32, s.shape, 1)
        parts = lanes(jnp.where(at < length - start, s, -1e30))
        before = m_ref[b]
        m = functools.reduce(jnp.maximum, parts, before)
        es = [jnp.exp2((c - m) * factor) for c in parts]
        for j, e in enumerate(es):
            e_ref[b + 1, :, j * 128 : (j + 1) * 128] = e
        m_ref[b + 1] = m
        l_ref[...] = l_ref[...] * jnp.exp2((before - m) * factor) + sum(es)

    last = m_ref[blocks]
    top = spread(jnp.max(last, axis=1, keepdims=True))
    total = jnp.sum(l_ref[...] * jnp.exp2((last - top) * factor), axis=1, keepdims=True)
    top_ref[...] = top
    inverse = spread(1.0 / total)
    l_ref[...] = inverse

    def probs(slot, n):
        scale = jnp.exp2((m_ref[slot] - top_ref[...]) * factor) * l_ref[...]
        return jnp.concatenate(
            [(e_ref[slot, :, j * 128 : (j + 1) * 128] * scale).astype(BF) for j in range(n)], axis=1
        )

    acc_ref[...] = jnp.dot(probs(0, new // 128), fresh_ref[1], preferred_element_type=jnp.float32)

    @pl.loop(0, blocks)
    def _(b):
        start = pl.multiple_of(b * block, block)
        acc_ref[...] += jnp.dot(
            probs(b + 1, block // 128), old_ref[slot, 1, pl.ds(start, block), :], preferred_element_type=jnp.float32
        )

    def write(out_ref):
        if with_kv:
            for k in range(2):
                cols = slice((heads + k) * HEAD_DIM, (heads + k + 1) * HEAD_DIM)
                out_ref[:, cols] = fresh_ref[k]
        for h in range(heads):
            out_ref[:, h * HEAD_DIM : (h + 1) * HEAD_DIM] = acc_ref[h * new : (h + 1) * new, :].astype(BF)

    if n_out == 1:
        write(out_refs[0])
    else:
        half = pl.num_programs(0) // 2
        pl.when(step < half)(lambda: write(out_refs[0]))
        pl.when(step >= half)(lambda: write(out_refs[1]))


def by_core(R, T, tokens, query_weight, key_weight, value_weight, cache_keys, cache_values, lengths, page_table):
    tok_rows, depth = tokens.shape
    shard = query_weight.shape[0]
    seqs = lengths.shape[1]
    new = tok_rows // seqs
    q_local = query_weight.shape[1] // T
    q_core = q_local // 2
    kv_width = key_weight.shape[1] // T
    r, z = lax.axis_index("rep"), lax.axis_index("tp")
    core = r % 2
    max_len = cache_keys.shape[1] * page_table.shape[2]

    def xor(a, bit):
        return lax.ppermute(a, "rep", [(i, i ^ bit) for i in range(R)])

    head_chunks = HEAD_CHUNKS
    widths = [(n + 2 * (c == 0)) * HEAD_DIM for c, n in enumerate(head_chunks)]
    firsts = [sum(widths[:c]) for c in range(len(widths))]
    own_firsts, col = {}, 0
    for c in OWN_ORDER:
        own_firsts[c] = col
        col += widths[c]
    whole = sum(widths)
    n_chunks = len(widths)

    starts = []
    for s in range(T):
        target = (z + s) % T
        for h in (core, 1 - core):
            starts += [target * q_local + h * q_core, target * kv_width + h * HEAD_DIM, target * kv_width + h * HEAD_DIM]
    for s in range(T):
        target = (z + s) % T
        for h in (core, 1 - core):
            base = target * q_local + h * q_core
            starts += [base + firsts[c] - 2 * HEAD_DIM if c else base for c in range(n_chunks)]
    starts = jnp.stack(starts).astype(jnp.int32)
    weights = (query_weight, key_weight, value_weight)

    def pieces(s, other, c, row, col):
        base, q_base = 3 * (2 * s + other), 6 * T + n_chunks * (2 * s + other)
        if c:
            return [(row, col, widths[c], 0, q_base + c)]
        return [
            (row, col, HEAD_DIM, 1, base + 1),
            (row, col + HEAD_DIM, HEAD_DIM, 2, base + 2),
        ] + ([(row, col + 2 * HEAD_DIM, widths[0] - 2 * HEAD_DIM, 0, q_base)] if head_chunks[0] else [])

    def all_chunks(s, other, row, col):
        return [p for c in range(n_chunks) for p in pieces(s, other, c, row, col + own_firsts[c])]

    def their_half(chunks):
        job, col, place = [], 0, {}
        for c in chunks:
            for s in range(1, T):
                job += pieces(s, 1, c, 0, col)
                place[s, c] = col
                col += widths[c]
        return pack([job], [(shard, col)], starts, weights, [])[0], place

    def to_send(got, place):
        jobs, shapes = [], []
        for s, c in place:
            jobs.append(pieces(s, 0, c, 0, 0) + [(shard, 0, widths[c], 3, place[s, c])])
            shapes.append((2 * shard, widths[c]))
        return dict(zip(place, pack(jobs, shapes, starts, weights, [got])))

    send_b, place_b = their_half([0])
    got_b = xor(send_b, 1)
    own_mine = pack([all_chunks(0, 0, 0, 0)], [(shard, whole)], starts, weights, [])[0]
    ready = to_send(got_b, place_b)
    send_a = pack([all_chunks(0, 1, 0, 0)], [(shard, whole)], starts, weights, [])[0]
    own_other = xor(send_a, 1)
    send_c, place_c = their_half(range(1, n_chunks))
    got_c = xor(send_c, 1)
    ready.update(to_send(got_c, place_c))

    def over_tp(c):
        got = []
        for s in range(1, T):
            got.append(lax.ppermute(ready[s, c], "tp", [(t, (t + s) % T) for t in range(T)]))
        rows = got[0].shape[0]
        jobs = [(k, 0, rows, 0, k * rows) for k in range(T - 1)]
        return move(jobs, got, [((T - 1) * rows, widths[c])])[0]

    def gather(piece):
        by_x, by_y = xor(piece, 2), xor(piece, 4)
        n = piece.shape[0] // 2
        jobs = [(0, 0, n, 0, 0), (1, n, n, 1, 0)]
        low, high = move(jobs, [by_y, by_x], [(n, piece.shape[1])] * 2)
        far = [(6, 0, xor(low, 2)), (6, n, xor(high, 4))]
        return [(0, 0, piece), (2, 0, by_x), (4, 0, by_y), *far]

    by_x, by_y = xor(own_mine, 2), xor(own_mine, 4)
    other_x, other_y = xor(own_other, 2), xor(own_other, 4)
    own_all = [
        (0, 0, own_mine), (0, shard, own_other), (2, 0, by_x), (2, shard, other_x), (4, 0, by_y),
        (4, shard, other_y), (6, 0, xor(by_y, 2)), (6, shard, xor(other_x, 4)),
    ]
    rest_all = [gather(over_tp(c)) for c in range(n_chunks)]

    their_tokens = xor(tokens, 1)
    seq_lengths = jnp.concatenate([xor(lengths, 1)[0], lengths[0]])
    old_shape = (2, seqs, max_len, HEAD_DIM)
    call = pl.pallas_call(
        pages_kernel,
        out_shape=[jax.ShapeDtypeStruct(old_shape, BF)] * 2,
        grid_spec=pltpu.PrefetchScalarGridSpec(
            num_scalar_prefetch=2,
            grid=(1,),
            in_specs=[pl.BlockSpec(memory_space=pl.ANY)] * 2,
            out_specs=[pl.BlockSpec(old_shape, lambda i, *_: (0, 0, 0, 0))] * 2,
            scratch_shapes=[pltpu.SemaphoreType.DMA((4 * seqs * page_table.shape[2],))],
        ),
        compiler_params=pltpu.CompilerParams(vmem_limit_bytes=VMEM_LIMIT),
        cost_estimate=pl.CostEstimate(flops=1000000, bytes_accessed=8000000, transcendentals=0),
        name="old",
    )
    my_old, for_them = call(core[None].astype(jnp.int32), page_table[0], cache_keys, cache_values)
    their_old = xor(for_them, 1)

    order, place = [], {}
    for shifts in ([0], list(range(1, T))):
        for d in range(0, R, 2):
            place[d, shifts[0]] = len(order)
            order += [(r ^ (d + e)) % 2 * T + (z - s) % T for s in shifts for e in range(2)]
    order = jnp.stack(order).astype(jnp.int32)
    chips = jnp.stack([(r ^ d) // 2 for d in range(0, R, 2)]).astype(jnp.int32)
    rows_all = 2 * tok_rows
    params = pltpu.CompilerParams(vmem_limit_bytes=VMEM_LIMIT)

    half = HEAD_DIM // 2
    frequency = ROPE_THETA ** (-2.0 * jnp.arange(half, dtype=jnp.float32) / HEAD_DIM)
    positions = (seq_lengths[:, None] + jnp.arange(new, dtype=jnp.int32)[None, :]).reshape(rows_all)
    angles = positions.astype(jnp.float32)[:, None] * frequency[None, :]
    cos, sin = jnp.cos(angles), jnp.sin(angles)
    cos, sin = jnp.concatenate([cos, cos], axis=1), jnp.concatenate([-sin, sin], axis=1)

    def attend(c, fresh, group=None, stage="all", before=None):
        ranks = range(R // 2)
        ranks = {"all": ranks, "before": ranks[:-1], "after": ranks[-1:]}[stage]
        n = head_chunks[c]
        width = n * HEAD_DIM
        with_kv = c == 0
        base = seqs * (group or 0)
        count = seqs if group is not None else 2 * seqs
        n_out = count // seqs
        block = KEY_BLOCK
        slots = max_len // block + 1
        m = max(n, 1) * new
        arrays, places = [], []
        for s, first, parts in ((0, own_firsts[c], own_all), (1, 0, rest_all[c])):
            for d, o, a in parts:
                if d // 2 in ranks:
                    arrays.append(a)
                    places.append((place[d, s] + o // shard, first, ranks.index(d // 2)))
        row = lambda i, *_: (i + base, 0)
        out_width = width + 2 * HEAD_DIM * with_kv
        out_shape = [jax.ShapeDtypeStruct((tok_rows, out_width), BF)] * n_out
        if n_out == 1:
            out_specs = [pl.BlockSpec((new, out_width), lambda i, *_: (i, 0))]
        else:
            out_specs = [
                pl.BlockSpec((new, out_width), lambda i, *_: (jnp.minimum(i, seqs - 1), 0)),
                pl.BlockSpec((new, out_width), lambda i, *_: (jnp.maximum(i - seqs, 0), 0)),
            ]
        fresh_spec = pl.BlockSpec((2, new, HEAD_DIM), lambda i, *_: (0, i + base, 0))
        if with_kv:
            out_shape.append(jax.ShapeDtypeStruct((2, rows_all, HEAD_DIM), BF))
            out_specs.append(fresh_spec)
        before_spec = pl.BlockSpec((new, widths[c]), row)
        if stage == "before":
            n_out, out_shape = 1, [jax.ShapeDtypeStruct((rows_all, widths[c]), jnp.float32)]
            out_specs = [before_spec]
        anywhere = pl.BlockSpec(memory_space=pl.ANY)
        call = pl.pallas_call(
            functools.partial(chunk_kernel, shard, places, ranks, stage, n, with_kv, block, base, n_out),
            out_shape=out_shape,
            grid_spec=pltpu.PrefetchScalarGridSpec(
                num_scalar_prefetch=3,
                grid=(count,),
                in_specs=[
                    pl.BlockSpec((new, HEAD_DIM), row),
                    pl.BlockSpec((new, HEAD_DIM), row),
                    *[anywhere] * 4,
                    *([before_spec] if stage == "after" else []),
                    *([] if with_kv or stage == "before" else [fresh_spec]),
                    *[anywhere] * len(arrays),
                ],
                out_specs=out_specs,
                scratch_shapes=[
                    pltpu.VMEM((2, new, len(ranks) * 2 * T * shard), BF),
                    pltpu.VMEM((len(ranks) * 2 * T * shard, widths[c]), BF),
                    pltpu.VMEM((2, 2, max_len, HEAD_DIM), BF),
                    pltpu.VMEM((m, HEAD_DIM), BF),
                    pltpu.VMEM((slots, m, block), jnp.float32),
                    pltpu.VMEM((slots, m, 128), jnp.float32),
                    pltpu.VMEM((m, 128), jnp.float32),
                    pltpu.VMEM((m, 128), jnp.float32),
                    pltpu.VMEM((m, 128), jnp.float32),
                    pltpu.SemaphoreType.DMA((2, 2 + len(ranks))),
                    pltpu.SemaphoreType.DMA((depth // shard,)),
                ],
            ),
            compiler_params=params,
            cost_estimate=pl.CostEstimate(
                flops=count * new * width * 2 * (depth + 2 * (max_len + new)),
                bytes_accessed=(count * new + width) * depth * 2,
                transcendentals=count * new * n * (max_len + new),
            ),
        )
        extra = () if with_kv or stage == "before" else (fresh,)
        extra = (before, *extra) if stage == "after" else extra
        return call(
            seq_lengths, order, chips, cos, sin, their_tokens, tokens, their_old, my_old, *extra, *arrays
        )

    out, at, fresh = jnp.zeros((tok_rows, q_local), BF), 0, None
    for c in range(n_chunks):
        if c in SPLIT:
            before = attend(c, None, stage="before")[0]
            theirs, mine = attend(c, fresh, stage="after", before=before)
        else:
            theirs, mine, *rest = attend(c, fresh)
        theirs = xor(theirs, 1)
        width = head_chunks[c] * HEAD_DIM
        if c == 0:
            fresh = rest[0]
            parts = []
            for k in range(2):
                cols = slice(width + k * HEAD_DIM, width + (k + 1) * HEAD_DIM)
                pair = (mine[:, cols], theirs[:, cols])
                parts.append(
                    jnp.concatenate([jnp.where(core == 0, *pair), jnp.where(core == 0, *pair[::-1])], axis=1)
                )
            new_cache = jnp.stack(parts)
        if not width:
            continue
        out = lax.dynamic_update_slice(out, mine[:, :width], (0, core * q_core + at))
        out = lax.dynamic_update_slice(out, theirs[:, :width], (0, (1 - core) * q_core + at))
        at += width
    return out, new_cache


def per_device(R, T, *args):
    _, query_weight, key_weight = args[:3]
    heads = query_weight.shape[1] // T // HEAD_DIM
    kv = key_weight.shape[1] // T // HEAD_DIM
    if R == 8 and kv == 2 and heads == 16:
        return by_core(R, T, *args)
    return plain(*args)


def solution(mesh):
    return jax.shard_map(
        functools.partial(per_device, mesh.shape["rep"], mesh.shape["tp"]),
        mesh=mesh,
        in_specs=(
            P("rep", None),
            P(("rep", "tp"), None),
            P(("rep", "tp"), None),
            P(("rep", "tp"), None),
            P("rep", None, "tp"),
            P("rep", None, "tp"),
            P("rep", None),
            P("rep", None, None),
        ),
        out_specs=(P("rep", "tp"), P(None, "rep", "tp")),
        check_vma=False,
    )
```
